8 devices in a mesh: fsdp: 8 (over z, y, x, core).
Axes of the slice: x: 2, y: 2, z: 1, core: 2. Of those that a mesh axis runs over, the one named last changes fastest.
Arguments:
- hidden: bfloat16 [4096, 2048], P('fsdp')
- positions: int32 [4096], P('fsdp')
- g_attn: float32 [2, 2048], replicated
- g_mlp: float32 [2, 2048], replicated
- w_q: bfloat16 [2, 2048, 2048], P(None, 'fsdp')
- w_k: bfloat16 [2, 2048, 2048], P(None, 'fsdp')
- w_v: bfloat16 [2, 2048, 2048], P(None, 'fsdp')
- w_o: bfloat16 [2, 2048, 2048], P(None, 'fsdp')
- w_gate: bfloat16 [2, 2048, 5632], P(None, 'fsdp')
- w_up: bfloat16 [2, 2048, 5632], P(None, 'fsdp')
- w_down: bfloat16 [2, 5632, 2048], P(None, 'fsdp')
- k_cache: bfloat16 [2, 4096, 8, 16, 128], P(None, 'fsdp')
- v_cache: bfloat16 [2, 4096, 8, 16, 128], P(None, 'fsdp')
Outputs:
- output 1: bfloat16 [4096, 2048], P('fsdp')
- output 2: bfloat16 [2, 4096, 8, 16, 128], P(None, 'fsdp')
- output 3: bfloat16 [2, 4096, 8, 16, 128], P(None, 'fsdp')
All inputs are finite; a program needn't handle non-finite values.
Results may differ from the reference program's by a relative error of at most 0.0155008.
Values are sent between devices in bfloat16 or wider.
A program may use at most 1 GiB of HBM per device.

```python
import jax
import jax.numpy as jnp
from jax import lax

D = 2048
HEADS = 16
HEAD = 128
FF = 5632
BATCH = 4096
SEQ = 8
LAYERS = 2
NORM_EPS = 1e-5
ROPE_THETA = 10000.0


def rms_norm(hidden_f32, gain_vec):
    mean_sq = jnp.mean(hidden_f32 * hidden_f32, axis=-1, keepdims=True)
    return (hidden_f32 * lax.rsqrt(mean_sq + NORM_EPS) * gain_vec).astype(jnp.bfloat16)


def rope_tables(positions):
    half_dim = HEAD // 2
    inv_freq = ROPE_THETA ** (-(jnp.arange(half_dim).astype(jnp.float32) * 2.0 / HEAD))
    angles = positions.astype(jnp.float32)[:, None] * inv_freq[None, :]
    return jnp.cos(angles)[:, None, :], jnp.sin(angles)[:, None, :]


def rotate(vec_f32, cos_tab, sin_tab):
    half_dim = HEAD // 2
    first_half = vec_f32[..., :half_dim]
    second_half = vec_f32[..., half_dim:]
    return jnp.concatenate([first_half * cos_tab - second_half * sin_tab, second_half * cos_tab + first_half * sin_tab], axis=-1)


def setup_inputs(seed: int = 0) -> dict:
    sub_keys = jax.random.split(jax.random.key(seed), 13)

    def weight(key_w, fan_in, fan_out):
        return (jax.random.normal(key_w, (LAYERS, fan_in, fan_out), jnp.float32) * fan_in ** -0.5).astype(jnp.bfloat16)

    positions = jax.random.randint(sub_keys[1], (BATCH,), 0, SEQ, jnp.int32).at[0].set(SEQ - 1)
    cache_shape = (LAYERS, BATCH, SEQ, HEADS, HEAD)
    return {
        "hidden": jax.random.normal(sub_keys[0], (BATCH, D), jnp.float32).astype(jnp.bfloat16),
        "positions": positions,
        "g_attn": jax.random.uniform(sub_keys[2], (LAYERS, D), jnp.float32, 0.5, 1.5),
        "g_mlp": jax.random.uniform(sub_keys[3], (LAYERS, D), jnp.float32, 0.5, 1.5),
        "w_q": weight(sub_keys[4], D, D),
        "w_k": weight(sub_keys[5], D, D),
        "w_v": weight(sub_keys[6], D, D),
        "w_o": weight(sub_keys[7], D, D),
        "w_gate": weight(sub_keys[8], D, FF),
        "w_up": weight(sub_keys[9], D, FF),
        "w_down": weight(sub_keys[10], FF, D),
        "k_cache": jax.random.normal(sub_keys[11], cache_shape, jnp.float32).astype(jnp.bfloat16),
        "v_cache": jax.random.normal(sub_keys[12], cache_shape, jnp.float32).astype(jnp.bfloat16),
    }


def reference(hidden, positions, g_attn, g_mlp, w_q, w_k, w_v, w_o, w_gate, w_up, w_down, k_cache, v_cache):
    cos_tab, sin_tab = rope_tables(positions)
    slot_ids = jnp.arange(SEQ)
    slot_hit = (slot_ids[None, :] == positions[:, None])[:, :, None, None]
    valid_mask = slot_ids[None, None, :] <= positions[:, None, None]

    def layer_step(hidden_in, params):
        attn_gain, mlp_gain, q_mat, k_mat, v_mat, o_mat, gate_mat, up_mat, down_mat, k_old, v_old = params
        resid_f32 = hidden_in.astype(jnp.float32)
        normed = rms_norm(resid_f32, attn_gain)
        q_rot = rotate(jnp.dot(normed, q_mat, preferred_element_type=jnp.float32).reshape(BATCH, HEADS, HEAD), cos_tab, sin_tab).astype(jnp.bfloat16)
        k_rot = rotate(jnp.dot(normed, k_mat, preferred_element_type=jnp.float32).reshape(BATCH, HEADS, HEAD), cos_tab, sin_tab).astype(jnp.bfloat16)
        v_new = jnp.dot(normed, v_mat, preferred_element_type=jnp.float32).reshape(BATCH, HEADS, HEAD).astype(jnp.bfloat16)
        k_all = jnp.where(slot_hit, k_rot[:, None], k_old)
        v_all = jnp.where(slot_hit, v_new[:, None], v_old)
        scores = jnp.einsum("bhd,bshd->bhs", q_rot.astype(jnp.float32), k_all.astype(jnp.float32)) * HEAD ** -0.5
        scores = jnp.where(valid_mask, scores, -1e30)
        exp_scores = jnp.exp(scores - jnp.max(scores, axis=-1, keepdims=True))
        prob_bf = (exp_scores / jnp.sum(exp_scores, axis=-1, keepdims=True)).astype(jnp.bfloat16)
        attn_mix = jnp.einsum("bhs,bshd->bhd", prob_bf.astype(jnp.float32), v_all.astype(jnp.float32)).astype(jnp.bfloat16).reshape(BATCH, D)
        after_attn = (resid_f32 + jnp.dot(attn_mix, o_mat, preferred_element_type=jnp.float32)).astype(jnp.bfloat16).astype(jnp.float32)
        normed_mlp = rms_norm(after_attn, mlp_gain)
        gate_pre = jnp.dot(normed_mlp, gate_mat, preferred_element_type=jnp.float32)
        up_pre = jnp.dot(normed_mlp, up_mat, preferred_element_type=jnp.float32)
        act_bf = (jax.nn.silu(gate_pre) * up_pre).astype(jnp.bfloat16)
        after_mlp = (after_attn + jnp.dot(act_bf, down_mat, preferred_element_type=jnp.float32)).astype(jnp.bfloat16)
        return after_mlp, (k_all, v_all)

    out_hidden, (k_out, v_out) = lax.scan(layer_step, hidden, (g_attn, g_mlp, w_q, w_k, w_v, w_o, w_gate, w_up, w_down, k_cache, v_cache))
    return out_hidden, k_out, v_out
```

```python
import functools

import jax
import jax.numpy as jnp
from jax import lax
from jax.experimental import pallas as pl
from jax.experimental.pallas import tpu as pltpu
from jax.sharding import PartitionSpec as P

AXIS_NAME = "fsdp"
HEAD_DIM = 128
NORM_EPS = 1e-5
ROPE_THETA = 10000.0
DEPTH = 2


def rms_norm(hidden_f32, gain_vec):
    mean_sq = jnp.mean(hidden_f32 * hidden_f32, axis=-1, keepdims=True)
    return (hidden_f32 * lax.rsqrt(mean_sq + NORM_EPS) * gain_vec).astype(jnp.bfloat16)


def rope_tables(positions):
    half_dim = HEAD_DIM // 2
    inv_freq = ROPE_THETA ** (-(jnp.arange(half_dim).astype(jnp.float32) * 2.0 / HEAD_DIM))
    angles = positions.astype(jnp.float32)[:, None] * inv_freq[None, :]
    cos_tab, sin_tab = jnp.cos(angles), jnp.sin(angles)
    return jnp.concatenate([cos_tab, cos_tab], axis=-1), jnp.concatenate([-sin_tab, sin_tab], axis=-1)


def swap(value, bit):
    return lax.ppermute(value, AXIS_NAME, [(i, i ^ bit) for i in range(8)])


class Link:
    def __init__(self, bit):
        self.bit, self.done = bit, []

    def send(self, value):
        if len(self.done) >= DEPTH:
            value, _ = lax.optimization_barrier((value, self.done[-DEPTH][:8, :128]))
        result = swap(value, self.bit)
        self.done.append(result)
        return result


def sibling(value):
    return swap(value, 1)


def block_sum(dev, x_ref, offs, w_refs):
    total = None
    for (rel, off), w_ref in zip(offs, w_refs):
        rows = w_ref.shape[0]
        start = pl.multiple_of((dev ^ rel) * 256 + off, 128)
        part = jnp.dot(x_ref[:, pl.ds(start, rows)], w_ref[...], preferred_element_type=jnp.float32)
        total = part if total is None else total + part
    return total


def qkv_body(offs, n_rot, dev_ref, x_ref, cos_ref, sin_ref, *refs):
    w_refs, o_ref = refs[:-1], refs[-1]
    total = block_sum(dev_ref[0], x_ref, offs, w_refs)
    step = pl.program_id(0)

    @pl.when(step < n_rot)
    def _():
        for head in range(total.shape[1] // HEAD_DIM):
            cols = slice(head * HEAD_DIM, (head + 1) * HEAD_DIM)
            vec = total[:, cols]
            rot = vec * cos_ref[...] + pltpu.roll(vec, HEAD_DIM // 2, 1) * sin_ref[...]
            o_ref[:, cols] = rot.astype(o_ref.dtype)

    @pl.when(step >= n_rot)
    def _():
        o_ref[...] = total.astype(o_ref.dtype)


def add_body(offs, dev_ref, x_ref, h_ref, *refs):
    w_refs, o_ref = refs[:-1], refs[-1]
    total = block_sum(dev_ref[0], x_ref, offs, w_refs)
    o_ref[...] = (h_ref[...].astype(jnp.float32) + total).astype(o_ref.dtype)


def gated_body(offs, dev_ref, x_ref, *refs):
    n = len(offs)
    gate = block_sum(dev_ref[0], x_ref, offs, refs[:n])
    up = block_sum(dev_ref[0], x_ref, offs, refs[n:2 * n])
    refs[-1][...] = (jax.nn.silu(gate) * up).astype(refs[-1].dtype)


def down_body(x_ref, w_ref, o_ref):
    o_ref[...] = jnp.dot(x_ref[...], w_ref[...], preferred_element_type=jnp.float32)


def cost(m, k, n, out_bytes):
    return pl.CostEstimate(flops=2 * m * k * n, bytes_accessed=2 * k * n + 2 * m * k + out_bytes * m * n, transcendentals=0)


PARAMS = pltpu.CompilerParams(vmem_limit_bytes=40 * 1024 * 1024)


def blocks_call(body, dev, x, extras, extra_specs, blocks, col_maps, n_out, tile, out_dtype):
    m, k = x.shape
    specs = [pl.BlockSpec((m, k), lambda j, d: (0, 0))] + extra_specs
    operands = [x] + extras
    for col_map in col_maps:
        for _, block in blocks:
            specs.append(pl.BlockSpec((block.shape[0], tile), col_map))
            operands.append(block)
    return pl.pallas_call(
        functools.partial(body, [key for key, _ in blocks]),
        grid_spec=pltpu.PrefetchScalarGridSpec(
            num_scalar_prefetch=1, grid=(n_out // tile,), in_specs=specs,
            out_specs=pl.BlockSpec((m, tile), lambda j, d: (0, j))),
        out_shape=jax.ShapeDtypeStruct((m, n_out), out_dtype),
        compiler_params=PARAMS, cost_estimate=cost(m, k, n_out * len(col_maps), 2),
    )(dev, *operands)


def qkv_call(dev, x, cos_tab, sin_tab, blocks, n_out):
    m = x.shape[0]
    tile = 512
    tab = pl.BlockSpec((m, HEAD_DIM), lambda j, d: (0, 0))

    def body(offs, *refs):
        qkv_body(offs, 2 * (n_out // 3) // tile, *refs)

    return blocks_call(body, dev, x, [cos_tab, sin_tab], [tab, tab], blocks, [lambda j, d: (0, j)], n_out, tile, jnp.bfloat16)


def o_call(dev, x, hidden, blocks):
    m, n_out = hidden.shape
    tile = 512
    return blocks_call(add_body, dev, x, [hidden], [pl.BlockSpec((m, tile), lambda j, d: (0, j))], blocks,
                       [lambda j, d: (0, j)], n_out, tile, jnp.bfloat16)


def gated_call(dev, x, blocks, n_out):
    tile = 256
    tiles = n_out // tile
    return blocks_call(gated_body, dev, x, [], [], blocks, [lambda j, d: (0, j), lambda j, d: (0, j + tiles)], n_out, tile, jnp.bfloat16)


def down_call(x, w):
    m, k = x.shape
    n_out = w.shape[1]
    tile = 512
    return pl.pallas_call(
        down_body, grid=(n_out // tile,),
        in_specs=[pl.BlockSpec((m, k), lambda j: (0, 0)), pl.BlockSpec((k, tile), lambda j: (0, j))],
        out_specs=pl.BlockSpec((m, tile), lambda j: (0, j)),
        out_shape=jax.ShapeDtypeStruct((m, n_out), jnp.float32),
        compiler_params=PARAMS, cost_estimate=cost(m, k, n_out, 4))(x, w)


def attn_body(rows, pos_ref, q_ref, kn_ref, vn_ref, kc_ref, vc_ref, *refs):
    o_ref, ko_ref, vo_ref = refs[-3:]
    base = pl.program_id(0) * rows
    n_slots = kc_ref.shape[2]

    def one_row(r, carry):
        pos = pos_ref[base + r]
        slots = lax.broadcasted_iota(jnp.int32, (n_slots, q_ref.shape[1], HEAD_DIM), 0)
        hit = slots == pos
        k_all = jnp.where(hit, kn_ref[r].astype(jnp.float32)[None], kc_ref[0, r].astype(jnp.float32))
        v_all = jnp.where(hit, vn_ref[r].astype(jnp.float32)[None], vc_ref[0, r].astype(jnp.float32))
        ko_ref[0, r] = k_all.astype(ko_ref.dtype)
        vo_ref[0, r] = v_all.astype(vo_ref.dtype)
        scores = jnp.sum(q_ref[r].astype(jnp.float32)[None] * k_all, axis=-1, keepdims=True) * HEAD_DIM ** -0.5
        scores = jnp.where(slots[:, :, :1] <= pos, scores, -1e30)
        exp_scores = jnp.exp(scores - jnp.max(scores, axis=0, keepdims=True))
        prob = (exp_scores / jnp.sum(exp_scores, axis=0, keepdims=True)).astype(jnp.bfloat16).astype(jnp.float32)
        o_ref[r] = jnp.sum(prob * v_all, axis=0).astype(o_ref.dtype)
        return carry

    lax.fori_loop(0, rows, one_row, 0, unroll=4)


def attn_call(layer, positions, q, k_new, v_new, k_cache, v_cache, outs):
    n_rows, n_heads, _ = q.shape
    rows = 32
    n_slots = k_cache.shape[2]
    vec = pl.BlockSpec((rows, n_heads, HEAD_DIM), lambda i, p: (i, 0, 0))
    cache = pl.BlockSpec((1, rows, n_slots, n_heads, HEAD_DIM), lambda i, p: (layer, i, 0, 0, 0))
    return pl.pallas_call(
        functools.partial(attn_body, rows),
        grid_spec=pltpu.PrefetchScalarGridSpec(
            num_scalar_prefetch=1, grid=(n_rows // rows,),
            in_specs=[vec, vec, vec, cache, cache] + [pl.BlockSpec(memory_space=pl.ANY)] * len(outs),
            out_specs=(vec, cache, cache)),
        out_shape=(jax.ShapeDtypeStruct(q.shape, jnp.bfloat16),
                   jax.ShapeDtypeStruct(k_cache.shape, k_cache.dtype), jax.ShapeDtypeStruct(v_cache.shape, v_cache.dtype)),
        input_output_aliases={6: 1, 7: 2} if outs else {},
        compiler_params=PARAMS,
        cost_estimate=pl.CostEstimate(flops=30_000_000_000, bytes_accessed=4 * k_cache.size // 2 * 2, transcendentals=0),
    )(positions, q, k_new, v_new, k_cache, v_cache, *outs)


def solution(mesh):
    def device_step(hidden, positions, g_attn, g_mlp, w_q, w_k, w_v, w_o, w_gate, w_up, w_down, k_cache, v_cache):
        index = lax.axis_index(AXIS_NAME)
        dev = index.astype(jnp.int32).reshape(1)
        x_pos = (index // 2) % 2
        n_rows, dim = hidden.shape
        n_layers = w_q.shape[0]
        n_heads = dim // HEAD_DIM
        quarter = w_gate.shape[2] // 4
        part = w_down.shape[1]
        x_link, y_link = Link(2), Link(4)

        def half_cols(mat, half):
            return [lax.dynamic_slice_in_dim(mat, half * quarter, quarter, 1),
                    lax.dynamic_slice_in_dim(mat, (2 + half) * quarter, quarter, 1)]

        weights = []
        for layer in range(n_layers):
            qkv = jnp.concatenate([w_q[layer], w_k[layer], w_v[layer]], axis=1)
            out = w_o[layer]
            mid = qkv.shape[0] // 2
            qkv_x, qkv_y = x_link.send(qkv), y_link.send(qkv)
            out_x, out_y = x_link.send(out), y_link.send(out)
            qkv_d1, qkv_d2 = y_link.send(qkv_x[:mid]), x_link.send(qkv_y[mid:])
            out_d1, out_d2 = y_link.send(out_x[:mid]), x_link.send(out_y[mid:])

            def eight(own, by_x, by_y, d1, d2):
                near = [((0, 0), own), ((2, 0), by_x), ((4, 0), by_y), ((6, 0), d1), ((6, mid), d2)]
                return near + [((rel + 1, off), sibling(block)) for (rel, off), block in near]

            keep = jnp.concatenate(half_cols(w_gate[layer], x_pos) + half_cols(w_up[layer], x_pos), axis=1)
            give = jnp.concatenate(half_cols(w_gate[layer], 1 - x_pos) + half_cols(w_up[layer], 1 - x_pos), axis=1)
            gu_x = x_link.send(give)
            gu_y = y_link.send(keep)
            gu_d = y_link.send(gu_x)
            down = w_down[layer]
            down_y = y_link.send(down)
            near = [((0, 0), keep), ((2, 0), gu_x), ((4, 0), gu_y), ((6, 0), gu_d)]
            gu_blocks = near + [((rel + 1, off), sibling(block)) for (rel, off), block in near]
            y_pos, core = index // 4, index % 2
            down_all = jnp.zeros((4 * part, dim), down.dtype)
            for block, slot in ((down, y_pos * 2 + core), (sibling(down), y_pos * 2 + 1 - core),
                                (down_y, (1 - y_pos) * 2 + core), (sibling(down_y), (1 - y_pos) * 2 + 1 - core)):
                down_all = lax.dynamic_update_slice_in_dim(down_all, block, slot * part, 0)
            weights.append((eight(qkv, qkv_x, qkv_y, qkv_d1, qkv_d2), eight(out, out_x, out_y, out_d1, out_d2), gu_blocks, down_all))

        cos_tab, sin_tab = rope_tables(positions)
        outs = ()
        for layer in range(n_layers):
            qkv_blocks, out_blocks, gu_blocks, down_all = weights[layer]
            normed = rms_norm(hidden.astype(jnp.float32), g_attn[layer])
            qkv = qkv_call(dev, normed, cos_tab, sin_tab, qkv_blocks, 3 * dim)
            q, k_new, v_new = (qkv[:, i * dim:(i + 1) * dim].reshape(n_rows, n_heads, HEAD_DIM) for i in range(3))
            mix, *outs = attn_call(layer, positions, q, k_new, v_new, k_cache, v_cache, outs)
            after_attn = o_call(dev, mix.reshape(n_rows, dim), hidden, out_blocks)
            normed_mlp = rms_norm(after_attn.astype(jnp.float32), g_mlp[layer])
            other_rows = swap(normed_mlp, 2)
            act = gated_call(dev, normed_mlp, gu_blocks, 2 * quarter)
            other_act = gated_call(dev, other_rows, gu_blocks, 2 * quarter)
            from_x = swap(down_call(other_act, down_all), 2)
            total = down_call(act, down_all) + from_x
            hidden = (after_attn.astype(jnp.float32) + total).astype(jnp.bfloat16)
        return hidden, *outs

    row_spec = P(AXIS_NAME, None)
    gain_spec = P(None, None)
    weight_spec = P(None, AXIS_NAME, None)
    cache_spec = P(None, AXIS_NAME, None, None, None)
    return jax.shard_map(
        device_step, mesh=mesh,
        in_specs=(row_spec, P(AXIS_NAME), gain_spec, gain_spec, weight_spec, weight_spec, weight_spec, weight_spec, weight_spec, weight_spec, weight_spec, cache_spec, cache_spec),
        out_specs=(row_spec, cache_spec, cache_spec),
        check_vma=False)
```
